128 devices in a mesh: fsdp: 16 (over y_hi, z, core), tensor: 8 (over y_lo, x).
Axes of the slice: x: 4, y: 4 (y_hi: 2, y_lo: 2; y = y_hi * 2 + y_lo), z: 4, core: 2. Of those that a mesh axis runs over, the one named last changes fastest.
Arguments:
- states: bfloat16 [4096, 8192], P('fsdp'), may hold values from -64 to 64
- segment_ids: int32 [16, 256], P('fsdp'), may hold values from 0 to 3, never falling along the last dimension, each value on 1 to 128 neighbouring positions
- attn_gain: float32 [8192], replicated, may hold values from 0.1 to 1.9
- query_weight: bfloat16 [8192, 4096], P('fsdp', 'tensor'), may hold values from -2 to 2
- key_weight: bfloat16 [8192, 1024], P('fsdp', 'tensor'), may hold values from -2 to 2
- value_matrix: bfloat16 [8192, 1024], P('fsdp', 'tensor'), may hold values from -0.0625 to 0.0625
- out_weight: bfloat16 [4096, 8192], P('tensor', 'fsdp'), may hold values from -0.28125 to 0.28125
- final_gain: float32 [8192], P('tensor'), may hold values from 0.1 to 1.9
- head_weight: float32 [8192], P('tensor'), may hold values from -0.0625 to 0.0625
Outputs:
- scores: float32 [4096], P(('fsdp', 'tensor'))
- resid_out: bfloat16 [4096, 8192], P('fsdp', 'tensor')
The draws below stay inside these ranges and needn't reach their ends.
Inputs may be any that keep to these rules, and one draw needn't show every extreme that they name: `segment_ids`: in each row, segment numbers never fall and each rollout spans 1 to 128 positions.
All inputs are finite; a program needn't handle non-finite values.
Results may differ from the reference program's by a relative error of at most 0.0071.
Values may be sent and summed in bfloat16 or wider, within the bound.
No kernel may reach another device: no remote copies, remote signals or barrier semaphores. Data moves between devices by JAX's collectives and lax.ppermute only.
A program may use at most 128 MiB of HBM per device.

```python
import math
import jax
import jax.numpy as jnp
import numpy as np
from jax import lax

MODEL_WIDTH = 8192
HQ = 32
KEY_VALUE_HEADS = 8
HEAD_SIZE = 128
TOK_DEV = 256
SEG_COUNT = 4
SEG_MOST = 128
TOKENS = 4096
N_FSDP = 16


def draw_states(key, part):
    subkeys = jax.random.split(jax.random.fold_in(key, 11), 1)
    noise_part = jnp.clip(jax.random.normal(subkeys[0], (TOKENS, MODEL_WIDTH), jnp.float32), -4.0, 4.0)
    col_scale = 3.0 ** (jnp.arange(MODEL_WIDTH, dtype=jnp.float32) / MODEL_WIDTH)
    return (noise_part * col_scale[None, :]).astype(jnp.bfloat16)


def matched_weight(key, heads, salt):
    subkeys = jax.random.split(jax.random.fold_in(key, salt), 1)
    drawn_part = jnp.clip(jax.random.normal(subkeys[0], (MODEL_WIDTH, heads * HEAD_SIZE), jnp.float32), -6.0, 6.0) * MODEL_WIDTH ** (-0.5)
    return drawn_part.astype(jnp.bfloat16)


def draw_query_weight(key, part):
    return matched_weight(key, HQ, 21)


def draw_key_weight(key, part):
    return matched_weight(key, KEY_VALUE_HEADS, 31)


def shard_levels(own_key, dims, shards, smallest, high):
    def one(dim, shards_of):
        steps = jax.random.uniform(jax.random.fold_in(jax.random.fold_in(own_key, 6), dim), (shards_of,), jnp.float32, smallest / len(shards), high / len(shards))
        return jnp.repeat(jnp.exp(steps), dims[dim] // shards_of).reshape((-1,) + (1,) * (len(dims) - dim - 1))

    gain = one(*shards[0])
    for cut in shards[1:]:
        gain = gain * one(*cut)
    return gain


def split_up(count, total, most, lean):
    weights = [(1 << 20) // math.isqrt(grade ** lean) + 1 for grade in range(2, count + 1)]
    surplus, counts = total - most - (count - 1), [1] * (count - 1)
    while surplus > 0:
        free = [i for i in range(count - 1) if counts[i] < most]
        pool, left = sum([weights[i] for i in free]), surplus
        for i in free:
            addition = min(most - counts[i], max(1, left * weights[i] // pool), surplus)
            counts[i] = counts[i] + addition
            surplus = surplus - addition
    return np.array([most] + counts)


def uneven_parts(stream_key, number_of, total, limit, lean):
    if number_of == 2:
        one = jax.random.randint(stream_key, (), max(1, total - limit), min(limit, total - 1) + 1)
        return jnp.stack([one, total - one])
    tallies = jnp.asarray(split_up(number_of, total, limit, lean), jnp.int32)
    twos = (number_of - 1) // 2
    donor, taker = tallies[1:1 + 2 * twos:2], tallies[2:2 + 2 * twos:2]
    margin = jnp.minimum(donor - 1, limit - taker)
    passed = jax.random.randint(jax.random.fold_in(stream_key, 1), (twos,), 0, 1 << 20) % (margin + 1)
    tallies = tallies.at[1:1 + 2 * twos:2].set(donor - passed).at[2:2 + 2 * twos:2].set(taker + passed)
    return tallies[jax.random.permutation(jax.random.fold_in(stream_key, 2), number_of)]


def bell_draw(key, shape, scale, limit, shards=(), kind=jnp.bfloat16):
    factor_of = shard_levels(key, shape, shards, -0.22, 0.18) if shards else 1.0
    entries = jax.random.normal(key, shape, jnp.float32) * scale * factor_of
    return jnp.minimum(jnp.maximum(entries, -limit), limit).astype(kind)


def setup_inputs(seed: int = 0) -> dict:
    splits = jax.random.split(jax.random.key(seed), 10)
    states = draw_states(jax.random.fold_in(splits[9], 71), 0)
    segment_ids = jax.vmap(lambda own: jnp.searchsorted(jnp.cumsum(uneven_parts(own, SEG_COUNT, TOK_DEV, SEG_MOST, 1)), jnp.arange(TOK_DEV), side="right"))(jax.random.split(splits[1], N_FSDP)).reshape((N_FSDP, TOK_DEV)).astype(jnp.int32)
    attn_gain = jnp.clip(1.0 + 0.18 * jax.random.normal(splits[2], (MODEL_WIDTH,), jnp.float32), 0.1, 1.9)
    query_weight = draw_query_weight(jax.random.fold_in(splits[9], 71), 0)
    key_weight = draw_key_weight(jax.random.fold_in(splits[9], 71), 0)
    value_matrix = bell_draw(splits[5], (MODEL_WIDTH, KEY_VALUE_HEADS * HEAD_SIZE), MODEL_WIDTH ** -0.5, 0.0625, ((0, 16), (1, 8)))
    out_weight = bell_draw(splits[6], (HQ * HEAD_SIZE, MODEL_WIDTH), (3.0 / (HQ * HEAD_SIZE) ** 0.5), 0.28125, ((0, 8), (1, 16)))
    final_gain = jnp.clip(1.0 + 0.18 * jax.random.normal(splits[7], (MODEL_WIDTH,), jnp.float32), 0.1, 1.9)
    head_weight = bell_draw(splits[8], (MODEL_WIDTH,), MODEL_WIDTH ** -0.5, 0.0625, ((0, 8),), jnp.float32)
    return dict(states=states, segment_ids=segment_ids, attn_gain=attn_gain, query_weight=query_weight, key_weight=key_weight, value_matrix=value_matrix, out_weight=out_weight, final_gain=final_gain, head_weight=head_weight)


EPS = 1e-05
THETA = 500000.0
NEG_FILL = -1e+30

def rope_tables(seg_row):
    count = seg_row.shape[0]
    places = jnp.arange(count, dtype=jnp.int32)
    boundary = jnp.concatenate([jnp.ones((1,), dtype=bool), seg_row[1:] != seg_row[:-1]])
    begins = lax.cummax(jnp.where(boundary, places, jnp.zeros_like(places)), axis=0)
    positions = (places - begins).astype(jnp.float32)
    half_width = HEAD_SIZE // 2
    frequency = THETA ** (-(2.0 * jnp.arange(half_width, dtype=jnp.float32)) / HEAD_SIZE)
    angles = positions[:, None] * frequency[None, :]
    return (jnp.cos(angles), jnp.sin(angles))

def rotated(block, cosine, sine_part):
    half_width = block.shape[-1] // 2
    first_half = block[..., :half_width]
    second_half = block[..., half_width:]
    cos_rows = cosine[:, None, :]
    sin_rows = sine_part[:, None, :]
    return jnp.concatenate([first_half * cos_rows - second_half * sin_rows, second_half * cos_rows + first_half * sin_rows], axis=-1)

def attend(queries, key_rows, values, seg_row):
    t_rows = queries.shape[0]
    heads_here = queries.shape[1] // HEAD_SIZE
    groups_here = key_rows.shape[1] // HEAD_SIZE
    ratio = heads_here // groups_here
    cosine, sine_part = rope_tables(seg_row)
    query_rot = rotated(queries.reshape(t_rows, heads_here, HEAD_SIZE), cosine, sine_part).astype(jnp.bfloat16)
    key_rot = rotated(key_rows.reshape(t_rows, groups_here, HEAD_SIZE), cosine, sine_part).astype(jnp.bfloat16)
    value_rows = values.astype(jnp.bfloat16).reshape(t_rows, groups_here, HEAD_SIZE)
    grouped = query_rot.reshape(t_rows, groups_here, ratio, HEAD_SIZE)
    logits = jnp.einsum('tkgd,skd->kgts', grouped.astype(jnp.float32), key_rot.astype(jnp.float32)) * HEAD_SIZE ** (-0.5)
    places = jnp.arange(t_rows, dtype=jnp.int32)
    allowed = (seg_row[:, None] == seg_row[None, :]) & (places[None, :] <= places[:, None])
    logits = jnp.where(allowed[None, None], logits, NEG_FILL)
    row_peak = lax.optimization_barrier(jnp.max(logits, axis=-1, keepdims=True))
    raised = jnp.exp(logits - row_peak)
    probabilities = (raised / lax.optimization_barrier(jnp.sum(raised, axis=-1, keepdims=True))).astype(jnp.bfloat16)
    mixed = jnp.einsum('kgts,skd->tkgd', probabilities.astype(jnp.float32), value_rows.astype(jnp.float32))
    return mixed.astype(jnp.bfloat16).reshape(t_rows, heads_here * HEAD_SIZE)

def reference(states, segment_ids, attn_gain, query_weight, key_weight, value_matrix, out_weight, final_gain, head_weight):
    widened = states.astype(jnp.float32)
    normed = (widened * lax.rsqrt(lax.optimization_barrier(jnp.sum(widened * widened, axis=1, keepdims=True)) / MODEL_WIDTH + EPS) * attn_gain[None, :]).astype(jnp.bfloat16)
    normed_blocks = normed.reshape(N_FSDP, TOK_DEV, MODEL_WIDTH)

    def single_block(operands):
        block_rows, seg_row = operands
        queries = jnp.dot(block_rows, query_weight, preferred_element_type=jnp.float32)
        key_rows = jnp.dot(block_rows, key_weight, preferred_element_type=jnp.float32)
        values = jnp.dot(block_rows, value_matrix, preferred_element_type=jnp.float32)
        return attend(queries, key_rows, values, seg_row)
    mixed = lax.map(single_block, (normed_blocks, segment_ids)).reshape(TOKENS, HQ * HEAD_SIZE)
    branch = jnp.dot(mixed, out_weight, preferred_element_type=jnp.float32)
    resid_out = (widened + branch).astype(jnp.bfloat16)
    stream = resid_out.astype(jnp.float32)
    squares = lax.optimization_barrier(jnp.sum(stream * stream, axis=1))
    products = lax.optimization_barrier(jnp.sum(stream * (final_gain * head_weight)[None, :], axis=1))
    scores = products * lax.rsqrt(squares / MODEL_WIDTH + EPS)
    return (scores, resid_out)
```

```python
import jax
import jax.numpy as jnp
from jax import lax
from jax.sharding import PartitionSpec as P

MODEL_WIDTH = 8192
HEAD_SIZE = 128
EPS = 1e-05
THETA = 500000.0
NEG_FILL = -1e30
AXES = ("fsdp", "tensor")
BF = jnp.bfloat16
F32 = jnp.float32


def pairs(move):
    out = []
    for f in range(16):
        for t in range(8):
            y_hi, z, core = f // 8, (f // 2) % 4, f % 2
            y_lo, x = t // 4, t % 4
            y_hi, z, core, y_lo, x = move(y_hi, z, core, y_lo, x)
            out.append((f * 8 + t, (((y_hi % 2) * 4 + z % 4) * 2 + core % 2) * 8 + (y_lo % 2) * 4 + x % 4))
    return out


def shift(value, dy=0, dz=0, dc=0, dl=0, dx=0):
    perm = pairs(lambda h, z, c, l, x: (h + dy, z + dz, c + dc, l + dl, x + dx))
    return lax.ppermute(value, AXES, perm)


def transposed(value):
    perm = pairs(lambda h, z, c, l, x: (l, x, c, h, z))
    return lax.ppermute(value, AXES, perm)


def rope_tables(seg_row):
    count = seg_row.shape[0]
    places = jnp.arange(count, dtype=jnp.int32)
    boundary = jnp.concatenate([jnp.ones((1,), dtype=bool), seg_row[1:] != seg_row[:-1]])
    begins = lax.cummax(jnp.where(boundary, places, jnp.zeros_like(places)), axis=0)
    positions = (places - begins).astype(F32)
    half_width = HEAD_SIZE // 2
    frequency = THETA ** (-(2.0 * jnp.arange(half_width, dtype=F32)) / HEAD_SIZE)
    angles = positions[:, None] * frequency[None, :]
    return (jnp.cos(angles), jnp.sin(angles))


def rotated(block, cosine, sine_part):
    half_width = block.shape[-1] // 2
    first_half = block[..., :half_width]
    second_half = block[..., half_width:]
    cos_rows = cosine[:, None, :]
    sin_rows = sine_part[:, None, :]
    return jnp.concatenate(
        [
            first_half * cos_rows - second_half * sin_rows,
            second_half * cos_rows + first_half * sin_rows,
        ],
        axis=-1,
    )


def attend(queries, key_rows, values, seg_row):
    t_rows = queries.shape[0]
    heads_here = queries.shape[1] // HEAD_SIZE
    groups_here = key_rows.shape[1] // HEAD_SIZE
    ratio = heads_here // groups_here
    cosine, sine_part = rope_tables(seg_row)
    query_rot = rotated(queries.reshape(t_rows, heads_here, HEAD_SIZE), cosine, sine_part).astype(BF)
    key_rot = rotated(key_rows.reshape(t_rows, groups_here, HEAD_SIZE), cosine, sine_part).astype(BF)
    value_rows = values.astype(BF).reshape(t_rows, groups_here, HEAD_SIZE)
    grouped = query_rot.reshape(t_rows, groups_here, ratio, HEAD_SIZE)
    logits = jnp.einsum("tkgd,skd->kgts", grouped, key_rot, preferred_element_type=F32) * HEAD_SIZE ** (-0.5)
    places = jnp.arange(t_rows, dtype=jnp.int32)
    allowed = (seg_row[:, None] == seg_row[None, :]) & (places[None, :] <= places[:, None])
    logits = jnp.where(allowed[None, None], logits, NEG_FILL)
    row_peak = jnp.max(logits, axis=-1, keepdims=True)
    raised = jnp.exp(logits - row_peak)
    probabilities = (raised / jnp.sum(raised, axis=-1, keepdims=True)).astype(BF)
    mixed = jnp.einsum("kgts,skd->tkgd", probabilities, value_rows, preferred_element_type=F32)
    return mixed.astype(BF).reshape(t_rows, heads_here * HEAD_SIZE)


def body(
    states,
    segment_ids,
    attn_gain,
    query_weight,
    key_weight,
    value_matrix,
    out_weight,
    final_gain,
    head_weight,
):
    t_rows, width = states.shape
    fsdp = lax.axis_index("fsdp")
    tensor = lax.axis_index("tensor")
    y_hi, z, core = fsdp // 8, (fsdp // 2) % 4, fsdp % 2
    y_lo, x = tensor // 4, tensor % 4
    half = query_weight.shape[0] // 2

    def gathered_q(w):
        a1, a3, b0 = shift(w, dz=1), shift(w, dz=-1), shift(w, dy=1)
        a2 = (shift(a1[:half], dz=1), shift(a3[half:], dz=-1))
        b1, b3 = shift(b0, dz=1), shift(b0, dz=-1)
        b2 = (shift(b1[:half], dz=1), shift(b3[half:], dz=-1))
        return {(0, 0): (w,), (0, 1): (a1,), (0, 3): (a3,), (1, 0): (b0,), (0, 2): a2, (1, 1): (b1,), (1, 3): (b3,), (1, 2): b2}

    def gathered_kv(w):
        a1, a3, b0 = shift(w, dz=1), shift(w, dz=-1), shift(w, dy=1)
        a2 = shift(w, dz=2)
        b1, b3 = shift(a1, dy=1), shift(a3, dy=1)
        b2 = shift(a2, dy=1)
        return {(0, 0): (w,), (0, 1): (a1,), (0, 3): (a3,), (1, 0): (b0,), (0, 2): (a2,), (1, 1): (b1,), (1, 3): (b3,), (1, 2): (b2,)}

    kv = jnp.concatenate([key_weight, value_matrix], axis=1)
    out_block = transposed(out_weight)
    q_shards = gathered_q(query_weight)
    kv_shards = gathered_kv(kv)

    widened = states.astype(F32)
    normed = (
        widened
        * lax.rsqrt(jnp.sum(widened * widened, axis=1, keepdims=True) / MODEL_WIDTH + EPS)
        * attn_gain[None, :]
    ).astype(BF)
    blocks = normed.reshape(t_rows, 8, 2, 512)
    mine = lax.dynamic_index_in_dim(blocks, core, 2, keepdims=False)
    theirs = lax.dynamic_index_in_dim(blocks, 1 - core, 2, keepdims=False)
    got = shift(theirs, dc=1)
    both = jnp.concatenate([mine, got], axis=0)

    q_acc = kv_acc = None
    for dy, k in ((0, 0), (0, 1), (0, 3), (1, 0), (0, 2), (1, 1), (1, 3), (1, 2)):
        source = ((y_hi + dy) % 2) * 4 + (z - k) % 4
        cols = lax.dynamic_index_in_dim(both, source, 1, keepdims=False)
        at = 0
        for piece in q_shards[(dy, k)]:
            part = jnp.dot(cols[:, at : at + piece.shape[0]], piece, preferred_element_type=F32)
            q_acc = part if q_acc is None else q_acc + part
            at += piece.shape[0]
        at = 0
        for piece in kv_shards[(dy, k)]:
            part = jnp.dot(cols[:, at : at + piece.shape[0]], piece, preferred_element_type=F32)
            kv_acc = part if kv_acc is None else kv_acc + part
            at += piece.shape[0]
    queries = q_acc[:t_rows] + shift(q_acc[t_rows:], dc=1)
    keys_values = kv_acc[:t_rows] + shift(kv_acc[t_rows:], dc=1)

    o1, o3, o2, p0 = shift(out_block, dz=1), shift(out_block, dz=-1), shift(out_block, dz=2), shift(out_block, dy=1)
    p1, p3, p2 = shift(p0, dz=1), shift(p0, dz=-1), shift(o2, dy=1)
    out_shards = {(0, 0): out_block, (0, 1): o1, (0, 3): o3, (0, 2): o2, (1, 0): p0, (1, 1): p1, (1, 3): p3, (1, 2): p2}
    own_out = jnp.zeros((8, 512, 512), BF)
    for (dy, k), w in out_shards.items():
        source = ((y_hi + dy) % 2) * 4 + (z - k) % 4
        own_out = lax.dynamic_update_index_in_dim(own_out, w, source, 0)
    other_out = shift(own_out, dc=1)

    mixed = attend(queries, keys_values[:, :HEAD_SIZE], keys_values[:, HEAD_SIZE:], segment_ids[0])
    own_acc = other_acc = None
    for dl, k in ((0, 0), (0, 1), (0, 3), (1, 0), (0, 2), (1, 1), (1, 3), (1, 2)):
        piece = mixed if (dl, k) == (0, 0) else shift(mixed, dl=dl, dx=k)
        source = ((y_lo + dl) % 2) * 4 + (x - k) % 4
        a = jnp.dot(piece, lax.dynamic_index_in_dim(own_out, source, 0, keepdims=False), preferred_element_type=F32)
        b = jnp.dot(piece, lax.dynamic_index_in_dim(other_out, source, 0, keepdims=False), preferred_element_type=F32)
        own_acc = a if own_acc is None else own_acc + a
        other_acc = b if other_acc is None else other_acc + b
    branch = jnp.concatenate(
        [jnp.where(core == 0, own_acc, other_acc), jnp.where(core == 0, other_acc, own_acc)], axis=1
    )
    slice_cols = width // 8
    own_cols = lax.dynamic_slice_in_dim(states, tensor * slice_cols, slice_cols, 1).astype(F32)
    resid_out = (own_cols + branch).astype(BF)
    stream = resid_out.astype(F32)
    squares = jnp.sum(stream * stream, axis=1)
    products = jnp.sum(stream * (final_gain * head_weight)[None, :], axis=1)
    share = t_rows // 8
    sums = jnp.stack([squares.reshape(8, share), products.reshape(8, share)], axis=1)
    totals = lax.all_to_all(sums, "tensor", 0, 0, tiled=True).sum(axis=0)
    scores = totals[1] * lax.rsqrt(totals[0] / MODEL_WIDTH + EPS)
    return (scores, resid_out)


def solution(mesh):
    placed = (
        P("fsdp", None),
        P("fsdp", None),
        P(),
        P("fsdp", "tensor"),
        P("fsdp", "tensor"),
        P("fsdp", "tensor"),
        P("tensor", "fsdp"),
        P("tensor"),
        P("tensor"),
    )
    return jax.shard_map(
        body,
        mesh=mesh,
        in_specs=placed,
        out_specs=(P(("fsdp", "tensor")), P("fsdp", "tensor")),
        check_vma=False,
    )
```

```python
import functools

import jax
import jax.numpy as jnp
from jax import lax
from jax.experimental import pallas as pl
from jax.experimental.pallas import tpu as pltpu
from jax.sharding import PartitionSpec as P

MODEL_WIDTH = 8192
HEAD_SIZE = 128
EPS = 1e-05
THETA = 500000.0
NEG_FILL = -1e30
AXES = ("fsdp", "tensor")
BF = jnp.bfloat16
F32 = jnp.float32


def pairs(move):
    out = []
    for f in range(16):
        for t in range(8):
            y_hi, z, core = f // 8, (f // 2) % 4, f % 2
            y_lo, x = t // 4, t % 4
            y_hi, z, core, y_lo, x = move(y_hi, z, core, y_lo, x)
            out.append((f * 8 + t, (((y_hi % 2) * 4 + z % 4) * 2 + core % 2) * 8 + (y_lo % 2) * 4 + x % 4))
    return out


def shift(value, dy=0, dz=0, dc=0, dl=0, dx=0):
    perm = pairs(lambda h, z, c, l, x: (h + dy, z + dz, c + dc, l + dl, x + dx))
    return lax.ppermute(value, AXES, perm)


def moved(value, move):
    return lax.ppermute(value, AXES, pairs(move))


VM = pl.BlockSpec(memory_space=pltpu.VMEM)
SM = pl.BlockSpec(memory_space=pltpu.SMEM)
LIMIT = 60 * 1024 * 1024


def norm_kernel(core_ref, s_ref, g_ref, mine_ref, theirs_ref):
    core = core_ref[0]
    x = s_ref[...].astype(F32)
    scale = lax.rsqrt(jnp.sum(x * x, axis=1, keepdims=True) / MODEL_WIDTH + EPS)
    for ref, flip in ((mine_ref, core), (theirs_ref, 1 - core)):
        for j in range(8):
            cols = pl.ds(pl.multiple_of((2 * j + flip) * 512, 512), 512)
            ref[j] = (s_ref[:, cols].astype(F32) * scale * g_ref[:, cols]).astype(BF)


def normed_halves(core, states, gain):
    rows, width = states.shape
    step = 32
    out = jax.ShapeDtypeStruct((8, rows, 512), BF)
    return pl.pallas_call(
        norm_kernel,
        grid_spec=pltpu.PrefetchScalarGridSpec(
            num_scalar_prefetch=1,
            grid=(rows // step,),
            in_specs=[
                pl.BlockSpec((step, width), lambda i, c: (i, 0)),
                pl.BlockSpec((1, width), lambda i, c: (0, 0)),
            ],
            out_specs=[pl.BlockSpec((8, step, 512), lambda i, c: (0, i, 0))] * 2,
        ),
        out_shape=(out, out),
        cost_estimate=pl.CostEstimate(flops=8 * 10**9, bytes_accessed=9 * 2**20, transcendentals=0),
        name="norm",
    )(core.reshape(1), states, gain.reshape(1, width))


def project_kernel(plan, first, where_ref, *refs):
    n = sum(len(p) for p in plan)
    x_ref, got_ref = refs[0], refs[1]
    w_refs = refs[2 : 2 + n]
    rest = refs[2 + n :]
    acc_refs = rest[:2] if not first else (None, None)
    own_ref, other_ref = rest[-2:]
    rows = own_ref.shape[0]
    for side, (lo, width) in enumerate(((0, 512), (512, 256))):
        for tile in range(0, width, 256):
            acc = None
            at = 0
            for j, pieces in enumerate(plan):
                both = jnp.concatenate([x_ref[where_ref[j]], got_ref[where_ref[j]]], axis=0)
                row = 0
                for kind, depth in pieces:
                    w = w_refs[at]
                    at += 1
                    if kind != side:
                        continue
                    part = jnp.dot(both[:, row : row + depth], w[:, tile : tile + 256], preferred_element_type=F32)
                    row += depth
                    acc = part if acc is None else acc + part
            cols = slice(lo + tile, lo + tile + 256)
            if first:
                own_ref[:, cols] = acc[:rows]
                other_ref[:, cols] = acc[rows:]
            else:
                own_ref[:, cols] = acc_refs[0][:, cols] + acc[:rows]
                other_ref[:, cols] = acc_refs[1][:, cols] + acc[rows:]


def project(where, mine, got, shards, acc=None):
    plan = tuple(tuple((kind, w.shape[0]) for kind, w in pieces) for pieces in shards)
    ws = [w for pieces in shards for _, w in pieces]
    rows = mine.shape[1]
    out = jax.ShapeDtypeStruct((rows, 768), F32)
    extra = [] if acc is None else list(acc)
    return pl.pallas_call(
        functools.partial(project_kernel, plan, acc is None),
        in_specs=[SM] + [VM] * (2 + len(ws) + len(extra)),
        out_specs=(VM, VM),
        out_shape=(out, out),
        compiler_params=pltpu.CompilerParams(vmem_limit_bytes=LIMIT // 2),
        cost_estimate=pl.CostEstimate(flops=2 * 512 * 2048 * 768, bytes_accessed=2**20, transcendentals=0),
    )(where, mine, got, *ws, *extra)


def attend_kernel(a_ref, b_ref, cos_ref, sin_ref, row_ref, col_ref, out_ref):
    rows = a_ref.shape[0]
    cosine, sine = cos_ref[...], sin_ref[...]

    def rotated(at):
        x = a_ref[:, at : at + HEAD_SIZE] + b_ref[:, at : at + HEAD_SIZE]
        return (x * cosine + pltpu.roll(x, HEAD_SIZE // 2, 1) * sine).astype(BF)

    keys = rotated(512)
    values = (a_ref[:, 640:] + b_ref[:, 640:]).astype(BF)
    t = lax.broadcasted_iota(jnp.int32, (rows, rows), 0)
    s = lax.broadcasted_iota(jnp.int32, (rows, rows), 1)
    allowed = (col_ref[...] == row_ref[...]) & (s <= t)
    for h in range(4):
        q = rotated(h * HEAD_SIZE)
        logits = lax.dot_general(q, keys, (((1,), (1,)), ((), ())), preferred_element_type=F32) * HEAD_SIZE ** (-0.5)
        logits = jnp.where(allowed, logits, NEG_FILL)
        raised = jnp.exp(logits - jnp.max(logits, axis=1, keepdims=True))
        weights = (raised / jnp.sum(raised, axis=1, keepdims=True)).astype(BF)
        out_ref[:, h * HEAD_SIZE : (h + 1) * HEAD_SIZE] = jnp.dot(weights, values, preferred_element_type=F32).astype(BF)


def attended(own, other, cosine, sine, seg_row):
    rows = own.shape[0]
    return pl.pallas_call(
        attend_kernel,
        in_specs=[VM] * 6,
        out_specs=VM,
        out_shape=jax.ShapeDtypeStruct((rows, 512), BF),
        compiler_params=pltpu.CompilerParams(vmem_limit_bytes=LIMIT // 2),
        cost_estimate=pl.CostEstimate(flops=4 * 10**9, bytes_accessed=2**20, transcendentals=0),
        name="attend",
    )(own, other, cosine, sine, seg_row.reshape(1, rows), seg_row.reshape(rows, 1))


def out_kernel(where_ref, *refs):
    mixed, own, other = refs[:8], refs[8:16], refs[16:24]
    states_ref, gain_ref, head_ref, resid_ref, sums_ref, table = refs[24:]
    core = where_ref[16]
    rows = states_ref.shape[0]
    for j in range(8):
        table[where_ref[j]] = mixed[j][...]
    squares = products = None
    for side, shards in ((0, own), (1, other)):
        for tile in range(0, 512, 256):
            acc = None
            for j in range(8):
                part = jnp.dot(table[where_ref[8 + j]], shards[j][:, tile : tile + 256], preferred_element_type=F32)
                acc = part if acc is None else acc + part
            first = core if side == 0 else 1 - core
            cols = pl.ds(pl.multiple_of(first * 512 + tile, 256), 256)
            resid = (states_ref[:, cols].astype(F32) + acc).astype(BF)
            resid_ref[:, cols] = resid
            stream = resid.astype(F32)
            sq = jnp.sum(stream * stream, axis=1, keepdims=True)
            pr = jnp.sum(stream * (gain_ref[:, cols] * head_ref[:, cols]), axis=1, keepdims=True)
            squares = sq if squares is None else squares + sq
            products = pr if products is None else products + pr
    lane = lax.broadcasted_iota(jnp.int32, (rows, 128), 1)
    spread = jnp.where(lane == 0, squares, jnp.where(lane == 1, products, 0.0))
    sums_ref[...] = jnp.transpose(spread)[:8]


def finished(where, mixed, own, other, states, final_gain, head_weight):
    rows = states.shape[0]
    return pl.pallas_call(
        out_kernel,
        in_specs=[SM] + [VM] * 27,
        out_specs=(VM, VM),
        out_shape=(jax.ShapeDtypeStruct((rows, 1024), BF), jax.ShapeDtypeStruct((8, rows), F32)),
        scratch_shapes=[pltpu.VMEM((8, rows, 512), BF)],
        compiler_params=pltpu.CompilerParams(vmem_limit_bytes=LIMIT // 2),
        cost_estimate=pl.CostEstimate(flops=2 * 256 * 4096 * 1024, bytes_accessed=2**20, transcendentals=0),
        name="finish",
    )(where, *mixed, *own, *other, states, final_gain.reshape(1, 1024), head_weight.reshape(1, 1024))


def rope_tables(seg_row):
    count = seg_row.shape[0]
    places = jnp.arange(count, dtype=jnp.int32)
    boundary = jnp.concatenate([jnp.ones((1,), dtype=bool), seg_row[1:] != seg_row[:-1]])
    begins = lax.cummax(jnp.where(boundary, places, jnp.zeros_like(places)), axis=0)
    positions = (places - begins).astype(F32)
    half_width = HEAD_SIZE // 2
    frequency = THETA ** (-(2.0 * jnp.arange(half_width, dtype=F32)) / HEAD_SIZE)
    angles = positions[:, None] * frequency[None, :]
    cosine, sine = jnp.cos(angles), jnp.sin(angles)
    return (jnp.concatenate([cosine, cosine], axis=1), jnp.concatenate([-sine, sine], axis=1))


def body(
    states,
    segment_ids,
    attn_gain,
    query_weight,
    key_weight,
    value_matrix,
    out_weight,
    final_gain,
    head_weight,
):
    t_rows, _ = states.shape
    fsdp = lax.axis_index("fsdp")
    tensor = lax.axis_index("tensor")
    y_hi, z, core = fsdp // 8, (fsdp // 2) % 4, fsdp % 2
    y_lo, x = tensor // 4, tensor % 4
    half = query_weight.shape[0] // 2
    seg_row = segment_ids[0]

    def chip(dy, k):
        return ((y_hi + dy) % 2) * 4 + (z - k) % 4

    w = query_weight
    qa1, qa3, qb0 = shift(w, dz=1), shift(w, dz=-1), shift(w, dy=1)
    kv = jnp.concatenate([key_weight, value_matrix], axis=1)
    ka1, ka3, kb0 = shift(kv, dz=1), shift(kv, dz=-1), shift(kv, dy=1)
    ka2 = shift(kv, dz=2)
    turned = moved(out_weight, lambda h, z, c, l, x: (l, z + x, c, h, x))
    out_block = moved(turned, lambda h, z, c, l, x: (h, z, c, l, z - x))

    mine, theirs = normed_halves(core, states, attn_gain)
    got = shift(theirs, dc=1)

    qa2t, qa2b = shift(qa1[:half], dz=1), shift(qa3[half:], dz=-1)
    qb1, qb3 = shift(qb0, dz=1), shift(qb0, dz=-1)
    kb1, kb3 = shift(ka1, dy=1), shift(ka3, dy=1)
    kb2 = shift(ka2, dy=1)
    qb2t, qb2b = shift(qa2t, dy=1), shift(qa2b, dy=1)

    near = ((0, 0), (0, 1), (0, 3), (1, 0))
    far = ((0, 2), (1, 1), (1, 3), (1, 2))
    where = jnp.stack([chip(*p) for p in near])
    acc = project(where, mine, got, [
        [(0, w), (1, kv)], [(0, qa1), (1, ka1)], [(0, qa3), (1, ka3)], [(0, qb0), (1, kb0)]
    ])
    where = jnp.stack([chip(*p) for p in far])
    own, other = project(where, mine, got, [
        [(0, qa2t), (0, qa2b), (1, ka2)], [(0, qb1), (1, kb1)], [(0, qb3), (1, kb3)],
        [(0, qb2t), (0, qb2b), (1, kb2)],
    ], acc)
    back = shift(other, dc=1)
    cosine, sine = rope_tables(seg_row)
    mixed = attended(own, back, cosine, sine, seg_row)

    o1, o3, o2 = shift(out_block, dz=1), shift(out_block, dz=-1), shift(out_block, dz=2)
    p0 = shift(out_block, dy=1)
    p1, p3, p2 = shift(p0, dz=1), shift(p0, dz=-1), shift(o2, dy=1)
    own_out = (out_block, o1, o3, o2, p0, p1, p3, p2)
    out_places = ((0, 0), (0, 1), (0, 3), (0, 2), (1, 0), (1, 1), (1, 3), (1, 2))
    other_out = [shift(a, dc=1) for a in own_out]

    ml = shift(mixed, dl=1)
    mx = [shift(mixed, dx=k) for k in (1, 3, 2)]
    mlx = [shift(ml, dx=k) for k in (1, 3, 2)]
    pieces = [mixed, ml, *mx, *mlx]
    peers = ((0, 0), (1, 0), (0, 1), (0, 3), (0, 2), (1, 1), (1, 3), (1, 2))
    from_peer = [((y_lo + dl) % 2) * 4 + (x - k) % 4 for dl, k in peers]
    where = jnp.stack(from_peer + [((y_hi + dy) % 2) * 4 + (z - k - x) % 4 for dy, k in out_places] + [core])
    cols = lax.dynamic_slice_in_dim(states, tensor * 1024, 1024, 1)
    resid_out, sums = finished(where, pieces, own_out, other_out, cols, final_gain, head_weight)
    share = t_rows // 8
    sums = jnp.transpose(sums[:2].reshape(2, 8, share), (1, 0, 2))
    totals = lax.all_to_all(sums, "tensor", 0, 0, tiled=True).sum(axis=0)
    scores = totals[1] * lax.rsqrt(totals[0] / MODEL_WIDTH + EPS)
    return (scores, resid_out)


def solution(mesh):
    placed = (
        P("fsdp", None),
        P("fsdp", None),
        P(),
        P("fsdp", "tensor"),
        P("fsdp", "tensor"),
        P("fsdp", "tensor"),
        P("tensor", "fsdp"),
        P("tensor"),
        P("tensor"),
    )

    return jax.shard_map(
        body,
        mesh=mesh,
        in_specs=placed,
        out_specs=(P(("fsdp", "tensor")), P("fsdp", "tensor")),
        check_vma=False,
    )
```

```python
import functools

import jax
import jax.numpy as jnp
from jax import lax
from jax.experimental import pallas as pl
from jax.experimental.pallas import tpu as pltpu
from jax.sharding import PartitionSpec as P

MODEL_WIDTH = 8192
HEAD_SIZE = 128
EPS = 1e-05
THETA = 500000.0
NEG_FILL = -1e30
AXES = ("fsdp", "tensor")
BF = jnp.bfloat16
F32 = jnp.float32


def pairs(move):
    out = []
    for f in range(16):
        for t in range(8):
            y_hi, z, core = f // 8, (f // 2) % 4, f % 2
            y_lo, x = t // 4, t % 4
            y_hi, z, core, y_lo, x = move(y_hi, z, core, y_lo, x)
            out.append((f * 8 + t, (((y_hi % 2) * 4 + z % 4) * 2 + core % 2) * 8 + (y_lo % 2) * 4 + x % 4))
    return out


def shift(value, dy=0, dz=0, dc=0, dl=0, dx=0):
    perm = pairs(lambda h, z, c, l, x: (h + dy, z + dz, c + dc, l + dl, x + dx))
    return lax.ppermute(value, AXES, perm)


def moved(value, move):
    return lax.ppermute(value, AXES, pairs(move))


VM = pl.BlockSpec(memory_space=pltpu.VMEM)
SM = pl.BlockSpec(memory_space=pltpu.SMEM)


def norm_kernel(core_ref, s_ref, g_ref, mine_ref, theirs_ref):
    core = core_ref[0]
    x = s_ref[...].astype(F32)
    scale = lax.rsqrt(jnp.sum(x * x, axis=1, keepdims=True) / MODEL_WIDTH + EPS)
    for ref, flip in ((mine_ref, core), (theirs_ref, 1 - core)):
        for j in range(8):
            cols = pl.ds(pl.multiple_of((2 * j + flip) * 512, 512), 512)
            ref[j] = (s_ref[:, cols].astype(F32) * scale * g_ref[:, cols]).astype(BF)


def normed_halves(core, states, gain):
    rows, width = states.shape
    step = 32
    out = jax.ShapeDtypeStruct((8, rows, 512), BF)
    return pl.pallas_call(
        norm_kernel,
        grid_spec=pltpu.PrefetchScalarGridSpec(
            num_scalar_prefetch=1,
            grid=(rows // step,),
            in_specs=[
                pl.BlockSpec((step, width), lambda i, c: (i, 0)),
                pl.BlockSpec((1, width), lambda i, c: (0, 0)),
            ],
            out_specs=[pl.BlockSpec((8, step, 512), lambda i, c: (0, i, 0))] * 2,
        ),
        out_shape=(out, out),
        compiler_params=pltpu.CompilerParams(vmem_limit_bytes=16 * 2**20),
        cost_estimate=pl.CostEstimate(flops=8 * 10**9, bytes_accessed=9 * 2**20, transcendentals=0),
        name="norm",
    )(core.reshape(1), states, gain.reshape(1, width))


def project_kernel(plan, first, where_ref, *refs):
    n = sum(len(p) for p in plan)
    x_ref, got_ref = refs[0], refs[1]
    w_refs = refs[2 : 2 + n]
    rest = refs[2 + n :]
    acc_refs = rest[:2] if not first else (None, None)
    own_ref, other_ref = rest[-2:]
    rows = own_ref.shape[0]
    for side, (lo, width) in enumerate(((0, 512), (512, 256))):
        for tile in range(0, width, 256):
            acc = None
            at = 0
            for j, pieces in enumerate(plan):
                both = jnp.concatenate([x_ref[where_ref[j]], got_ref[where_ref[j]]], axis=0)
                row = 0
                for kind, depth in pieces:
                    w = w_refs[at]
                    at += 1
                    if kind != side:
                        continue
                    part = jnp.dot(both[:, row : row + depth], w[:, tile : tile + 256], preferred_element_type=F32)
                    row += depth
                    acc = part if acc is None else acc + part
            cols = slice(lo + tile, lo + tile + 256)
            if first:
                own_ref[:, cols] = acc[:rows]
                other_ref[:, cols] = acc[rows:]
            else:
                own_ref[:, cols] = acc_refs[0][:, cols] + acc[:rows]
                other_ref[:, cols] = acc_refs[1][:, cols] + acc[rows:]


def project(where, mine, got, shards, acc=None):
    plan = tuple(tuple((kind, w.shape[0]) for kind, w in pieces) for pieces in shards)
    ws = [w for pieces in shards for _, w in pieces]
    rows = mine.shape[1]
    out = jax.ShapeDtypeStruct((rows, 768), F32)
    extra = [] if acc is None else list(acc)
    return pl.pallas_call(
        functools.partial(project_kernel, plan, acc is None),
        in_specs=[SM] + [VM] * (2 + len(ws) + len(extra)),
        out_specs=(VM, VM),
        out_shape=(out, out),
        compiler_params=pltpu.CompilerParams(vmem_limit_bytes=16 * 2**20),
        cost_estimate=pl.CostEstimate(flops=2 * 512 * 2048 * 768, bytes_accessed=2**20, transcendentals=0),
    )(where, mine, got, *ws, *extra)


def attend_kernel(a_ref, b_ref, cos_ref, sin_ref, row_ref, col_ref, out_ref):
    rows = a_ref.shape[0]
    cosine, sine = cos_ref[...], sin_ref[...]

    def rotated(at):
        x = a_ref[:, at : at + HEAD_SIZE] + b_ref[:, at : at + HEAD_SIZE]
        return (x * cosine + pltpu.roll(x, HEAD_SIZE // 2, 1) * sine).astype(BF)

    keys = rotated(512)
    values = (a_ref[:, 640:] + b_ref[:, 640:]).astype(BF)
    t = lax.broadcasted_iota(jnp.int32, (rows, rows), 0)
    s = lax.broadcasted_iota(jnp.int32, (rows, rows), 1)
    allowed = (col_ref[...] == row_ref[...]) & (s <= t)
    for h in range(4):
        q = rotated(h * HEAD_SIZE)
        logits = lax.dot_general(q, keys, (((1,), (1,)), ((), ())), preferred_element_type=F32) * HEAD_SIZE ** (-0.5)
        logits = jnp.where(allowed, logits, NEG_FILL)
        raised = jnp.exp(logits - jnp.max(logits, axis=1, keepdims=True))
        weights = (raised / jnp.sum(raised, axis=1, keepdims=True)).astype(BF)
        out_ref[:, h * HEAD_SIZE : (h + 1) * HEAD_SIZE] = jnp.dot(weights, values, preferred_element_type=F32).astype(BF)


def attended(own, other, cosine, sine, seg_row):
    rows = own.shape[0]
    return pl.pallas_call(
        attend_kernel,
        in_specs=[VM] * 6,
        out_specs=VM,
        out_shape=jax.ShapeDtypeStruct((rows, 512), BF),
        compiler_params=pltpu.CompilerParams(vmem_limit_bytes=16 * 2**20),
        cost_estimate=pl.CostEstimate(flops=4 * 10**9, bytes_accessed=2**20, transcendentals=0),
        name="attend",
    )(own, other, cosine, sine, seg_row.reshape(1, rows), seg_row.reshape(rows, 1))


def part_kernel(where_ref, *refs):
    mixed, weights = refs[:5], refs[5:21]
    held_ref, acc_ref, sems = refs[21:]
    copies = [pltpu.make_async_copy(ref, held_ref.at[j], sems.at[j]) for j, ref in enumerate(weights)]
    for copy in copies:
        copy.start()
    for side in range(2):
        for copy in copies[8 * side : 8 * side + 8]:
            copy.wait()
        for tile in range(0, 512, 256):
            acc = None
            for j in range(5):
                block = held_ref[8 * side + where_ref[j], :, tile : tile + 256]
                part = jnp.dot(mixed[j][...], block, preferred_element_type=F32)
                acc = part if acc is None else acc + part
            acc_ref[:, 512 * side + tile : 512 * side + tile + 256] = acc


def partial_out(where, mixed, weights):
    rows = mixed[0].shape[0]
    return pl.pallas_call(
        part_kernel,
        in_specs=[SM] + [VM] * 5 + [pl.BlockSpec(memory_space=pl.ANY)] * 16,
        out_specs=(VM, VM),
        out_shape=(jax.ShapeDtypeStruct((16, 512, 512), BF), jax.ShapeDtypeStruct((rows, 1024), F32)),
        scratch_shapes=[pltpu.SemaphoreType.DMA((16,))],
        compiler_params=pltpu.CompilerParams(vmem_limit_bytes=20 * 2**20),
        cost_estimate=pl.CostEstimate(flops=2 * 256 * 4096 * 1024, bytes_accessed=2**20, transcendentals=0),
        name="part",
    )(where, *mixed, *weights)


def out_kernel(where_ref, *refs):
    mixed, held_ref, acc_ref = refs[:3], refs[3], refs[4]
    states_ref, gain_ref, head_ref, resid_ref, sums_ref = refs[5:]
    core = where_ref[8]
    squares = products = None
    for side in range(2):
        first = core if side == 0 else 1 - core
        for tile in range(0, 512, 256):
            acc = acc_ref[:, 512 * side + tile : 512 * side + tile + 256]
            for j in range(3):
                block = held_ref[8 * side + where_ref[5 + j], :, tile : tile + 256]
                acc = acc + jnp.dot(mixed[j][...], block, preferred_element_type=F32)
            cols = pl.ds(pl.multiple_of(first * 512 + tile, 256), 256)
            resid = (states_ref[:, cols].astype(F32) + acc).astype(BF)
            resid_ref[:, cols] = resid
            stream = resid.astype(F32)
            sq = stream * stream
            pr = stream * (gain_ref[:, cols] * head_ref[:, cols])
            sq = sq[:, :128] + sq[:, 128:]
            pr = pr[:, :128] + pr[:, 128:]
            squares = sq if squares is None else squares + sq
            products = pr if products is None else products + pr
    sums_ref[0:1] = jnp.sum(jnp.transpose(squares), axis=0, keepdims=True)
    sums_ref[1:2] = jnp.sum(jnp.transpose(products), axis=0, keepdims=True)


def finished(where, mixed, held, acc, states, final_gain, head_weight):
    rows = states.shape[0]
    return pl.pallas_call(
        out_kernel,
        in_specs=[SM] + [VM] * 8,
        out_specs=(VM, VM),
        out_shape=(jax.ShapeDtypeStruct((rows, 1024), BF), jax.ShapeDtypeStruct((2, rows), F32)),
        compiler_params=pltpu.CompilerParams(vmem_limit_bytes=20 * 2**20),
        cost_estimate=pl.CostEstimate(flops=2 * 256 * 1536 * 1024, bytes_accessed=2**20, transcendentals=0),
        name="finish",
    )(where, *mixed, held, acc, states, final_gain.reshape(1, 1024), head_weight.reshape(1, 1024))


def rope_tables(seg_row):
    count = seg_row.shape[0]
    places = jnp.arange(count, dtype=jnp.int32)
    boundary = jnp.concatenate([jnp.ones((1,), dtype=bool), seg_row[1:] != seg_row[:-1]])
    begins = lax.cummax(jnp.where(boundary, places, jnp.zeros_like(places)), axis=0)
    positions = (places - begins).astype(F32)
    half_width = HEAD_SIZE // 2
    frequency = THETA ** (-(2.0 * jnp.arange(half_width, dtype=F32)) / HEAD_SIZE)
    angles = positions[:, None] * frequency[None, :]
    cosine, sine = jnp.cos(angles), jnp.sin(angles)
    return (jnp.concatenate([cosine, cosine], axis=1), jnp.concatenate([-sine, sine], axis=1))


STAGES = (((0, 0), (0, 1), (0, 3), (1, 0)), ((0, 2), (1, 1), (1, 3)), ((1, 2),))


def body(
    states,
    segment_ids,
    attn_gain,
    query_weight,
    key_weight,
    value_matrix,
    out_weight,
    final_gain,
    head_weight,
):
    t_rows, _ = states.shape
    fsdp = lax.axis_index("fsdp")
    tensor = lax.axis_index("tensor")
    y_hi, z, core = fsdp // 8, (fsdp // 2) % 4, fsdp % 2
    y_lo, x = tensor // 4, tensor % 4
    half = query_weight.shape[0] // 2
    seg_row = segment_ids[0]

    def chip(dy, k):
        return ((y_hi + dy) % 2) * 4 + (z - k) % 4

    w = query_weight
    qa1, qa3, qb0 = shift(w, dz=1), shift(w, dz=-1), shift(w, dy=1)
    kv = jnp.concatenate([key_weight, value_matrix], axis=1)
    ka1, ka3, kb0 = shift(kv, dz=1), shift(kv, dz=-1), shift(kv, dy=1)
    ka2 = shift(kv, dz=2)
    turned = moved(out_weight, lambda h, z, c, l, x: (l, z + x, c, h, x))
    out_block = moved(turned, lambda h, z, c, l, x: (h, z, c, l, z - x))

    mine, theirs = normed_halves(core, states, attn_gain)
    got = shift(theirs, dc=1)

    qa2t, qa2b = shift(qa1[:half], dz=1), shift(qa3[half:], dz=-1)
    qb1, qb3 = shift(qb0, dz=1), shift(qb0, dz=-1)
    kb1, kb3 = shift(ka1, dy=1), shift(ka3, dy=1)
    kb2 = shift(ka2, dy=1)
    qb2t, qb2b = shift(qa2t, dy=1), shift(qa2b, dy=1)

    shards = {
        (0, 0): [(0, w), (1, kv)],
        (0, 1): [(0, qa1), (1, ka1)],
        (0, 3): [(0, qa3), (1, ka3)],
        (1, 0): [(0, qb0), (1, kb0)],
        (0, 2): [(0, qa2t), (0, qa2b), (1, ka2)],
        (1, 1): [(0, qb1), (1, kb1)],
        (1, 3): [(0, qb3), (1, kb3)],
        (1, 2): [(0, qb2t), (0, qb2b), (1, kb2)],
    }
    acc = None
    for places in STAGES:
        where = jnp.stack([chip(*p) for p in places])
        rows_mine, rows_got = mine, got
        if len(places) == 1:
            rows_mine = lax.dynamic_slice_in_dim(mine, where[0], 1, 0)
            rows_got = lax.dynamic_slice_in_dim(got, where[0], 1, 0)
            where = jnp.zeros((1,), jnp.int32)
        acc = project(where, rows_mine, rows_got, [shards[p] for p in places], acc)
    own, other = acc
    back = shift(other, dc=1)
    cosine, sine = rope_tables(seg_row)
    mixed = attended(own, back, cosine, sine, seg_row)

    o1, o3, o2 = shift(out_block, dz=1), shift(out_block, dz=-1), shift(out_block, dz=2)
    p0 = shift(out_block, dy=1)
    p1, p3, p2 = shift(p0, dz=1), shift(p0, dz=-1), shift(o2, dy=1)
    own_out = (out_block, o1, o3, o2, p0, p1, p3, p2)
    other_out = [shift(a, dc=1) for a in own_out]

    ml = shift(mixed, dl=1)
    mx = [shift(mixed, dx=k) for k in (1, 3, 2)]
    mlx = [shift(ml, dx=k) for k in (1, 3, 2)]
    pieces = [mixed, ml, *mx, *mlx]
    peers = ((0, 0), (1, 0), (0, 1), (0, 3), (0, 2), (1, 1), (1, 3), (1, 2))
    places = []
    for dl, k in peers:
        turn = (z - x - (x - k)) % 4
        places.append(((y_lo + dl - y_hi) % 2) * 4 + (turn ^ (turn >> 1)))
    where = jnp.stack(places + [core])
    held, early = partial_out(where, pieces[:5], (*own_out, *other_out))
    cols = lax.dynamic_slice_in_dim(states, tensor * 1024, 1024, 1)
    resid_out, sums = finished(where, pieces[5:], held, early, cols, final_gain, head_weight)
    share = t_rows // 8
    sums = jnp.transpose(sums.reshape(2, 8, share), (1, 0, 2))
    totals = lax.all_to_all(sums, "tensor", 0, 0, tiled=True).sum(axis=0)
    scores = totals[1] * lax.rsqrt(totals[0] / MODEL_WIDTH + EPS)
    return (scores, resid_out)


def solution(mesh):
    placed = (
        P("fsdp", None),
        P("fsdp", None),
        P(),
        P("fsdp", "tensor"),
        P("fsdp", "tensor"),
        P("fsdp", "tensor"),
        P("tensor", "fsdp"),
        P("tensor"),
        P("tensor"),
    )

    return jax.shard_map(
        body,
        mesh=mesh,
        in_specs=placed,
        out_specs=(P(("fsdp", "tensor")), P("fsdp", "tensor")),
        check_vma=False,
    )
```

```python
import functools

import jax
import jax.numpy as jnp
from jax import lax
from jax.experimental import pallas as pl
from jax.experimental.pallas import tpu as pltpu
from jax.sharding import PartitionSpec as P

MODEL_WIDTH = 8192
HEAD_SIZE = 128
EPS = 1e-05
THETA = 500000.0
NEG_FILL = -1e30
AXES = ("fsdp", "tensor")
BF = jnp.bfloat16
F32 = jnp.float32


def pairs(move):
    out = []
    for f in range(16):
        for t in range(8):
            y_hi, z, core = f // 8, (f // 2) % 4, f % 2
            y_lo, x = t // 4, t % 4
            y_hi, z, core, y_lo, x = move(y_hi, z, core, y_lo, x)
            out.append((f * 8 + t, (((y_hi % 2) * 4 + z % 4) * 2 + core % 2) * 8 + (y_lo % 2) * 4 + x % 4))
    return out


def shift(value, dy=0, dz=0, dc=0, dl=0, dx=0):
    perm = pairs(lambda h, z, c, l, x: (h + dy, z + dz, c + dc, l + dl, x + dx))
    return lax.ppermute(value, AXES, perm)


def moved(value, move):
    return lax.ppermute(value, AXES, pairs(move))


VM = pl.BlockSpec(memory_space=pltpu.VMEM)
SM = pl.BlockSpec(memory_space=pltpu.SMEM)


def norm_kernel(core_ref, s_ref, g_ref, mine_ref, theirs_ref):
    core = core_ref[0]
    x = s_ref[...].astype(F32)
    scale = lax.rsqrt(jnp.sum(x * x, axis=1, keepdims=True) / MODEL_WIDTH + EPS)
    for ref, flip in ((mine_ref, core), (theirs_ref, 1 - core)):
        for j in range(8):
            cols = pl.ds(pl.multiple_of((2 * j + flip) * 512, 512), 512)
            ref[j] = (s_ref[:, cols].astype(F32) * scale * g_ref[:, cols]).astype(BF)


def normed_halves(core, states, gain):
    rows, width = states.shape
    step = 32
    out = jax.ShapeDtypeStruct((8, rows, 512), BF)
    return pl.pallas_call(
        norm_kernel,
        grid_spec=pltpu.PrefetchScalarGridSpec(
            num_scalar_prefetch=1,
            grid=(rows // step,),
            in_specs=[
                pl.BlockSpec((step, width), lambda i, c: (i, 0)),
                pl.BlockSpec((1, width), lambda i, c: (0, 0)),
            ],
            out_specs=[pl.BlockSpec((8, step, 512), lambda i, c: (0, i, 0))] * 2,
        ),
        out_shape=(out, out),
        compiler_params=pltpu.CompilerParams(vmem_limit_bytes=16 * 2**20),
        cost_estimate=pl.CostEstimate(flops=8 * 10**9, bytes_accessed=9 * 2**20, transcendentals=0),
        name="norm",
    )(core.reshape(1), states, gain.reshape(1, width))


def copy_kernel(moves, *refs):
    ins, out_ref, sems = refs[:-2], refs[-2], refs[-1]
    copies = [
        pltpu.make_async_copy(ref.at[rows, :], out_ref.at[:, cols], sems.at[i])
        for i, (ref, (rows, cols)) in enumerate(zip(ins, moves))
    ]
    for copy in copies:
        copy.start()
    for copy in copies:
        copy.wait()


def side_by_side(arrays, start, rows):
    moves, at = [], 0
    for a in arrays:
        moves.append((pl.ds(start, rows), pl.ds(at, a.shape[1])))
        at += a.shape[1]
    return pl.pallas_call(
        functools.partial(copy_kernel, moves),
        in_specs=[pl.BlockSpec(memory_space=pltpu.HBM)] * len(arrays),
        out_specs=VM,
        out_shape=jax.ShapeDtypeStruct((rows, at), arrays[0].dtype),
        scratch_shapes=[pltpu.SemaphoreType.DMA((len(arrays),))],
        compiler_params=pltpu.CompilerParams(vmem_limit_bytes=8 * 2**20),
        cost_estimate=pl.CostEstimate(flops=10**8, bytes_accessed=2**20, transcendentals=0),
    )(*arrays)


def project_kernel(depths, first, where_ref, *refs):
    n = sum(len(d) for d in depths)
    x_ref, got_ref = refs[0], refs[1]
    w_refs = refs[2 : 2 + n]
    acc_refs = refs[2 + n : -2]
    own_ref, other_ref = refs[-2:]
    rows = own_ref.shape[0]
    for tile in range(0, 768, 256):
        cols = slice(tile, tile + 256)
        acc = None
        at = 0
        for j, pieces in enumerate(depths):
            both = jnp.concatenate([x_ref[where_ref[j]], got_ref[where_ref[j]]], axis=0)
            row = 0
            for depth in pieces:
                part = jnp.dot(both[:, row : row + depth], w_refs[at][:, cols], preferred_element_type=F32)
                at += 1
                row += depth
                acc = part if acc is None else acc + part
        if first:
            own_ref[:, cols] = acc[:rows]
            other_ref[:, cols] = acc[rows:]
        else:
            own_ref[:, cols] = acc_refs[0][:, cols] + acc[:rows]
            other_ref[:, cols] = acc_refs[1][:, cols] + acc[rows:]


def project(where, mine, got, shards, acc=None):
    depths = tuple(tuple(w.shape[0] for w in pieces) for pieces in shards)
    ws = [w for pieces in shards for w in pieces]
    rows = mine.shape[1]
    out = jax.ShapeDtypeStruct((rows, 768), F32)
    extra = [] if acc is None else list(acc)
    return pl.pallas_call(
        functools.partial(project_kernel, depths, acc is None),
        in_specs=[SM] + [VM] * (2 + len(ws) + len(extra)),
        out_specs=(VM, VM),
        out_shape=(out, out),
        compiler_params=pltpu.CompilerParams(vmem_limit_bytes=16 * 2**20),
        cost_estimate=pl.CostEstimate(flops=2 * 512 * 2048 * 768, bytes_accessed=2**20, transcendentals=0),
    )(where, mine, got, *ws, *extra)


def attend_kernel(a_ref, b_ref, cos_ref, sin_ref, row_ref, col_ref, out_ref):
    rows = a_ref.shape[0]
    cosine, sine = cos_ref[...], sin_ref[...]

    def rotated(at):
        x = a_ref[:, at : at + HEAD_SIZE] + b_ref[:, at : at + HEAD_SIZE]
        return (x * cosine + pltpu.roll(x, HEAD_SIZE // 2, 1) * sine).astype(BF)

    keys = rotated(512)
    values = (a_ref[:, 640:] + b_ref[:, 640:]).astype(BF)
    t = lax.broadcasted_iota(jnp.int32, (rows, rows), 0)
    s = lax.broadcasted_iota(jnp.int32, (rows, rows), 1)
    allowed = (col_ref[...] == row_ref[...]) & (s <= t)
    for h in range(4):
        q = rotated(h * HEAD_SIZE)
        logits = lax.dot_general(q, keys, (((1,), (1,)), ((), ())), preferred_element_type=F32) * HEAD_SIZE ** (-0.5)
        logits = jnp.where(allowed, logits, NEG_FILL)
        raised = jnp.exp(logits - jnp.max(logits, axis=1, keepdims=True))
        weights = (raised / jnp.sum(raised, axis=1, keepdims=True)).astype(BF)
        out_ref[:, h * HEAD_SIZE : (h + 1) * HEAD_SIZE] = jnp.dot(weights, values, preferred_element_type=F32).astype(BF)


def attended(own, other, cosine, sine, seg_row):
    rows = own.shape[0]
    return pl.pallas_call(
        attend_kernel,
        in_specs=[VM] * 6,
        out_specs=VM,
        out_shape=jax.ShapeDtypeStruct((rows, 512), BF),
        compiler_params=pltpu.CompilerParams(vmem_limit_bytes=16 * 2**20),
        cost_estimate=pl.CostEstimate(flops=4 * 10**9, bytes_accessed=2**20, transcendentals=0),
        name="attend",
    )(own, other, cosine, sine, seg_row.reshape(1, rows), seg_row.reshape(rows, 1))


def part_kernel(where_ref, *refs):
    mixed, weights = refs[:5], refs[5:21]
    held_ref, acc_ref, sems = refs[21:]
    copies = [pltpu.make_async_copy(ref, held_ref.at[j], sems.at[j]) for j, ref in enumerate(weights)]
    for copy in copies:
        copy.start()
    for side in range(2):
        for copy in copies[8 * side : 8 * side + 8]:
            copy.wait()
        for tile in range(0, 512, 256):
            acc = None
            for j in range(5):
                block = held_ref[8 * side + where_ref[j], :, tile : tile + 256]
                part = jnp.dot(mixed[j][...], block, preferred_element_type=F32)
                acc = part if acc is None else acc + part
            acc_ref[:, 512 * side + tile : 512 * side + tile + 256] = acc


def partial_out(where, mixed, weights):
    rows = mixed[0].shape[0]
    return pl.pallas_call(
        part_kernel,
        in_specs=[SM] + [VM] * 5 + [pl.BlockSpec(memory_space=pl.ANY)] * 16,
        out_specs=(VM, VM),
        out_shape=(jax.ShapeDtypeStruct((16, 512, 512), BF), jax.ShapeDtypeStruct((rows, 1024), F32)),
        scratch_shapes=[pltpu.SemaphoreType.DMA((16,))],
        compiler_params=pltpu.CompilerParams(vmem_limit_bytes=20 * 2**20),
        cost_estimate=pl.CostEstimate(flops=2 * 256 * 4096 * 1024, bytes_accessed=2**20, transcendentals=0),
        name="part",
    )(where, *mixed, *weights)


def out_kernel(where_ref, *refs):
    mixed, held_ref, acc_ref = refs[:3], refs[3], refs[4]
    states_ref, gain_ref, head_ref, resid_ref, sums_ref = refs[5:]
    core = where_ref[8]
    squares = products = None
    for side in range(2):
        first = core if side == 0 else 1 - core
        for tile in range(0, 512, 256):
            acc = acc_ref[:, 512 * side + tile : 512 * side + tile + 256]
            for j in range(3):
                block = held_ref[8 * side + where_ref[5 + j], :, tile : tile + 256]
                acc = acc + jnp.dot(mixed[j][...], block, preferred_element_type=F32)
            cols = pl.ds(pl.multiple_of(first * 512 + tile, 256), 256)
            resid = (states_ref[:, cols].astype(F32) + acc).astype(BF)
            resid_ref[:, cols] = resid
            stream = resid.astype(F32)
            sq = stream * stream
            pr = stream * (gain_ref[:, cols] * head_ref[:, cols])
            sq = sq[:, :128] + sq[:, 128:]
            pr = pr[:, :128] + pr[:, 128:]
            squares = sq if squares is None else squares + sq
            products = pr if products is None else products + pr
    sums_ref[0:1] = jnp.sum(jnp.transpose(squares), axis=0, keepdims=True)
    sums_ref[1:2] = jnp.sum(jnp.transpose(products), axis=0, keepdims=True)


def finished(where, mixed, held, acc, states, final_gain, head_weight):
    rows = states.shape[0]
    return pl.pallas_call(
        out_kernel,
        in_specs=[SM] + [VM] * 8,
        out_specs=(VM, VM),
        out_shape=(jax.ShapeDtypeStruct((rows, 1024), BF), jax.ShapeDtypeStruct((2, rows), F32)),
        compiler_params=pltpu.CompilerParams(vmem_limit_bytes=20 * 2**20),
        cost_estimate=pl.CostEstimate(flops=2 * 256 * 1536 * 1024, bytes_accessed=2**20, transcendentals=0),
        name="finish",
    )(where, *mixed, held, acc, states, final_gain.reshape(1, 1024), head_weight.reshape(1, 1024))


def rope_tables(seg_row):
    count = seg_row.shape[0]
    places = jnp.arange(count, dtype=jnp.int32)
    boundary = jnp.concatenate([jnp.ones((1,), dtype=bool), seg_row[1:] != seg_row[:-1]])
    begins = lax.cummax(jnp.where(boundary, places, jnp.zeros_like(places)), axis=0)
    positions = (places - begins).astype(F32)
    half_width = HEAD_SIZE // 2
    frequency = THETA ** (-(2.0 * jnp.arange(half_width, dtype=F32)) / HEAD_SIZE)
    angles = positions[:, None] * frequency[None, :]
    cosine, sine = jnp.cos(angles), jnp.sin(angles)
    return (jnp.concatenate([cosine, cosine], axis=1), jnp.concatenate([-sine, sine], axis=1))


STAGES = (((0, 0), (0, 1), (0, 3), (1, 0)), ((0, 2), (1, 1), (1, 3)), ((1, 2),))


def body(
    states,
    segment_ids,
    attn_gain,
    query_weight,
    key_weight,
    value_matrix,
    out_weight,
    final_gain,
    head_weight,
):
    t_rows, _ = states.shape
    fsdp = lax.axis_index("fsdp")
    tensor = lax.axis_index("tensor")
    y_hi, z, core = fsdp // 8, (fsdp // 2) % 4, fsdp % 2
    y_lo, x = tensor // 4, tensor % 4
    half = query_weight.shape[0] // 2
    seg_row = segment_ids[0]

    def chip(dy, k):
        return ((y_hi + dy) % 2) * 4 + (z - k) % 4

    w = side_by_side([query_weight, key_weight, value_matrix], 0, 2 * half)
    a1, a3, b0 = shift(w, dz=1), shift(w, dz=-1), shift(w, dy=1)
    turned = moved(out_weight, lambda h, z, c, l, x: (l, z + x, c, h, x))
    out_block = moved(turned, lambda h, z, c, l, x: (h, z, c, l, z - x))

    mine, theirs = normed_halves(core, states, attn_gain)
    got = shift(theirs, dc=1)

    a2t, a2b = shift(a1[:half], dz=1), shift(a3[half:], dz=-1)
    b1, b3 = shift(b0, dz=1), shift(b0, dz=-1)
    b2t, b2b = shift(a2t, dy=1), shift(a2b, dy=1)
    shards = {
        (0, 0): [w],
        (0, 1): [a1],
        (0, 3): [a3],
        (1, 0): [b0],
        (0, 2): [a2t, a2b],
        (1, 1): [b1],
        (1, 3): [b3],
        (1, 2): [b2t, b2b],
    }
    acc = None
    for places in STAGES:
        where = jnp.stack([chip(*p) for p in places])
        rows_mine, rows_got = mine, got
        if len(places) == 1:
            rows_mine = lax.dynamic_slice_in_dim(mine, where[0], 1, 0)
            rows_got = lax.dynamic_slice_in_dim(got, where[0], 1, 0)
            where = jnp.zeros((1,), jnp.int32)
        acc = project(where, rows_mine, rows_got, [shards[p] for p in places], acc)
    own, other = acc
    back = shift(other, dc=1)
    cosine, sine = rope_tables(seg_row)
    mixed = attended(own, back, cosine, sine, seg_row)

    o1, o3, o2 = shift(out_block, dz=1), shift(out_block, dz=-1), shift(out_block, dz=2)
    p0 = shift(out_block, dy=1)
    p1, p3, p2 = shift(p0, dz=1), shift(p0, dz=-1), shift(o2, dy=1)
    own_out = (out_block, o1, o3, o2, p0, p1, p3, p2)
    other_out = [shift(a, dc=1) for a in own_out]

    ml = shift(mixed, dl=1)
    mx = [shift(mixed, dx=k) for k in (1, 3, 2)]
    mlx = [shift(ml, dx=k) for k in (1, 3, 2)]
    pieces = [mixed, ml, *mx, *mlx]
    peers = ((0, 0), (1, 0), (0, 1), (0, 3), (0, 2), (1, 1), (1, 3), (1, 2))
    places = []
    for dl, k in peers:
        turn = (z - x - (x - k)) % 4
        places.append(((y_lo + dl - y_hi) % 2) * 4 + (turn ^ (turn >> 1)))
    where = jnp.stack(places + [core])
    held, early = partial_out(where, pieces[:5], (*own_out, *other_out))
    cols = lax.dynamic_slice_in_dim(states, tensor * 1024, 1024, 1)
    resid_out, sums = finished(where, pieces[5:], held, early, cols, final_gain, head_weight)
    share = t_rows // 8
    sums = jnp.transpose(sums.reshape(2, 8, share), (1, 0, 2))
    totals = lax.all_to_all(sums, "tensor", 0, 0, tiled=True).sum(axis=0)
    scores = totals[1] * lax.rsqrt(totals[0] / MODEL_WIDTH + EPS)
    return (scores, resid_out)


def solution(mesh):
    placed = (
        P("fsdp", None),
        P("fsdp", None),
        P(),
        P("fsdp", "tensor"),
        P("fsdp", "tensor"),
        P("fsdp", "tensor"),
        P("tensor", "fsdp"),
        P("tensor"),
        P("tensor"),
    )

    return jax.shard_map(
        body,
        mesh=mesh,
        in_specs=placed,
        out_specs=(P(("fsdp", "tensor")), P("fsdp", "tensor")),
        check_vma=False,
    )
```
